256 devices in a mesh: grp: 4 (over y), col: 64 (over x, z, core).
Axes of the slice: x: 4, y: 4, z: 8, core: 2. Of those that a mesh axis runs over, the one named last changes fastest.
Arguments:
- panels: bfloat16 [256, 4, 512, 512], P('col', None, 'grp'), may hold values from -1.296875 to 1.296875
- parent: float32 [256, 512, 512], P('col', 'grp'), may hold values from -6 to 6
- src_block: int32 [64, 40], P('col'), may hold values from 0 to 39, each once within a row
- dest_owner: int32 [2560, 1], P('col'), may hold values from 0 to 63; in each aligned block of 40 rows (0 to 39, 40 to 79, ...) no two rows name the same one
- target: int32 [2560], P('col'), may hold values from 0 to 3
- counts: int32 [64], P('col'), may hold values from 20 to 40, as said below
Outputs:
- assembled: float32 [256, 512, 512], P('col', 'grp')
The draws below stay inside these ranges and needn't reach their ends.
Inputs may be any that keep to these rules, and one draw needn't show every extreme that they name: `src_block`: each row of a column rank is a permutation of the 40 block pairs. `dest_owner`: among the 40 slots of one column rank at most 1 name the same owner. The live slots of a rank are its first counts[c]; some rank has all 40 live.
All inputs are finite; a program needn't handle non-finite values.
Results may differ from the reference program's by a relative error of at most 0.0026.
Values may be sent and summed in bfloat16 or wider, within the bound.
No kernel may reach another device: no remote copies, remote signals or barrier semaphores. Data moves between devices by JAX's collectives and lax.ppermute only.
A program may use at most 128 MiB of HBM per device.

```python
import math
import jax
import jax.numpy as jnp
import numpy as np
from jax import lax

WIDTH = 512
BLOCK = 512
ROW_BLOCKS = 4
FRONTS = 4
TARGETS = 4
PAIRS = 10
SLOTS = 40
CAPACITY = 1
N_COL = 64


def draw_counts(key, part):
    values = jax.random.randint(key, (N_COL,), SLOTS // 2, SLOTS + 1).astype(jnp.int32)
    chosen = jax.random.randint(jax.random.fold_in(key, 7), (), 0, N_COL)
    return values.at[chosen].set(SLOTS)


def set_ends(drawn, own_key, least, high):
    index_at = [jax.random.randint(jax.random.fold_in(own_key, axis), (), 0, length) for axis, length in enumerate(drawn.shape)]
    widest = drawn.shape.index(max(drawn.shape))
    next_to = index_at[:widest] + [(index_at[widest] + 1) % drawn.shape[widest]] + index_at[widest + 1:]
    return drawn.at[tuple(index_at)].set(least).at[tuple(next_to)].set(high)


def level_of(stream_key, shape, cuts, low, top_value):
    def one(position, shards_of):
        steps = jax.random.uniform(jax.random.fold_in(jax.random.fold_in(stream_key, 6), position), (shards_of,), jnp.float32, low / len(cuts), top_value / len(cuts))
        return jnp.repeat(jnp.exp(steps), shape[position] // shards_of).reshape((-1,) + (1,) * (len(shape) - position - 1))

    factor_of = one(*cuts[0])
    for cut in cuts[1:]:
        factor_of = factor_of * one(*cut)
    return factor_of


def shared_out(stream_key, own, number, rows, amount, top, bound, slope):
    ranking = jax.random.permutation(stream_key, amount)
    crowded, common = load_shares(amount, rows * top, bound, slope, True), load_shares(amount, rows * top, bound, slope, False)
    places = jnp.arange(amount)

    def named(lengths, turn):
        used = int((lengths > 0).sum())
        fixed = max(1, used // 4)
        passed = fixed + (places - fixed + turn * (used - fixed)) % max(1, amount - fixed)
        return jnp.zeros((amount,), jnp.int32).at[ranking[jnp.where(places < fixed, places, passed)]].set(jnp.asarray(lengths, jnp.int32))

    lengths = jnp.where(number % 4 == 0, named(crowded, number // 4), named(common, number - number // 4 - 1))
    mixed = jax.random.permutation(jax.random.fold_in(own, 3), amount)
    giver, sink = mixed[0:amount // 2 * 2:2], mixed[1:amount // 2 * 2:2]
    slack = jnp.minimum(lengths[giver] - 1, bound - lengths[sink]) // 2
    slack = jnp.where((giver == ranking[0]) | (sink == ranking[0]) | (lengths[sink] == 0), 0, jnp.maximum(slack, 0))
    passed = jax.random.randint(jax.random.fold_in(own, 4), (amount // 2,), 0, 1 << 20) % (slack + 1)
    lengths = lengths.at[giver].add(-passed).at[sink].add(passed)
    members = jnp.searchsorted(jnp.cumsum(lengths), jnp.arange(rows * top), side="right").astype(jnp.int32)
    listing = members.reshape(top, rows).T
    listing = listing[jax.random.permutation(jax.random.fold_in(own, 1), rows)]
    turn = jax.random.randint(jax.random.fold_in(own, 2), (rows, 1), 0, top)
    return jnp.take_along_axis(listing, (jnp.arange(top)[None, :] + turn) % top, axis=1)


def load_shares(amount, total, most, skew, full):
    portions = [(1 << 20) // math.isqrt(rank ** skew) + 1 for rank in range(1, amount + 1)]
    largest = most if full else min(most, max(-(-total // amount), total * portions[0] // sum(portions)))
    least = 1 if total - largest >= amount - 1 else 0
    given, rest = [largest] + [least] * (amount - 1), total - largest - least * (amount - 1)
    while rest > 0:
        candidates = [i for i in range(1, amount) if given[i] < largest] or [i for i in range(1, amount) if given[i] < most]
        whole, remaining = sum([portions[i] for i in candidates]), rest
        for i in candidates:
            addition = min(most - given[i], max(1, remaining * portions[i] // whole), rest)
            given[i] = given[i] + addition
            rest = rest - addition
    return np.array(given)


def centred(stream_key, shape, spread, most, shards=(), kind=jnp.bfloat16):
    result = jax.random.normal(stream_key, shape, jnp.float32) * spread
    if len(shards) > 0:
        result = level_of(stream_key, shape, shards, -0.22, 0.18) * result
    return jnp.clip(result, min=-most, max=most).astype(kind)


def setup_inputs(seed: int = 0) -> dict:
    streams_of = jax.random.split(jax.random.key(seed), 7)
    panels = centred(streams_of[0], (N_COL * FRONTS, ROW_BLOCKS, BLOCK, WIDTH), 0.21, 1.296875, ((0, 64), (2, 4)))
    parent = centred(streams_of[1], (N_COL * TARGETS, BLOCK, BLOCK), 1.0, 6.0, ((0, 64), (1, 4)), jnp.float32)
    src_block = jax.vmap(lambda own: jax.random.permutation(own, SLOTS))(jax.random.split(streams_of[2], N_COL)).reshape((N_COL, SLOTS)).astype(jnp.int32)
    dest_owner_keys = jax.random.split(jax.random.fold_in(streams_of[3], 1), (N_COL * SLOTS) // SLOTS)
    dest_owner_turns = jax.random.permutation(jax.random.fold_in(streams_of[3], 3), (N_COL * SLOTS) // SLOTS)
    dest_owner = jax.vmap(lambda own, number: shared_out(jax.random.fold_in(streams_of[3], 2), own, number, SLOTS, N_COL, 1, CAPACITY, 2))(dest_owner_keys, dest_owner_turns).reshape((N_COL * SLOTS, 1))
    target = set_ends(jax.random.randint(streams_of[4], (N_COL * SLOTS,), 0, TARGETS), jax.random.fold_in(streams_of[4], 1), 0, TARGETS - 1).astype(jnp.int32)
    counts = draw_counts(jax.random.fold_in(streams_of[6], 71), 0)
    return dict(panels=panels, parent=parent, src_block=src_block, dest_owner=dest_owner, target=target, counts=counts)


def reference(panels, parent, src_block, dest_owner, target, counts):
    running = parent.astype(jnp.float32)
    slot_index = jnp.arange(SLOTS, dtype=jnp.int32)
    upper_table = jnp.asarray(np.array([a for a in range(ROW_BLOCKS) for b in range(a + 1)], np.int32))
    lower_table = jnp.asarray(np.array([b for a in range(ROW_BLOCKS) for b in range(a + 1)], np.int32))

    def add_device(column_rank, running):
        own_panels = lax.dynamic_slice_in_dim(panels, (column_rank * FRONTS).astype(jnp.int32), FRONTS, 0)
        flat_rows = own_panels.astype(jnp.float32).reshape(FRONTS * ROW_BLOCKS, BLOCK, WIDTH)
        combos = lax.dynamic_index_in_dim(src_block, column_rank, 0, keepdims=False)
        front_of = combos // PAIRS
        within = combos % PAIRS
        left_index = (front_of * ROW_BLOCKS + upper_table[within]).astype(jnp.int32)
        right_index = (front_of * ROW_BLOCKS + lower_table[within]).astype(jnp.int32)
        left_rows = flat_rows[left_index]
        right_rows = flat_rows[right_index]
        updates = jnp.einsum("srw,scw->src", left_rows, right_rows, precision=lax.Precision.HIGHEST)
        updates = updates.astype(jnp.bfloat16).astype(jnp.float32)
        limit = lax.dynamic_index_in_dim(counts, column_rank, 0, keepdims=False)
        is_live = slot_index < limit
        updates = jnp.where(is_live[:, None, None], updates, jnp.zeros_like(updates))
        start = (column_rank * SLOTS).astype(jnp.int32)
        owner_rank = lax.dynamic_slice_in_dim(dest_owner[:, 0], start, SLOTS, 0)
        block_target = lax.dynamic_slice_in_dim(target, start, SLOTS, 0)
        dest_rows = (owner_rank * TARGETS + block_target).astype(jnp.int32)
        return running.at[dest_rows].add(-updates)

    return lax.fori_loop(0, N_COL, add_device, running)
```

```python
import functools

import jax
import jax.numpy as jnp
from jax import lax
from jax.experimental import pallas as pl
from jax.experimental.pallas import tpu as pltpu
from jax.sharding import Mesh, PartitionSpec as P


NX, NZ, NC, NY = 4, 8, 2, 4
FRONTS, BLOCKS, ROWS, WIDTH = 4, 4, 128, 512
PAIRS, SLOTS, TARGETS = 10, 40, 4
COLS = 128
SPOTS = NX * NC * NZ
LABEL_ROWS = 16
SENT_ROWS = NZ * ROWS + LABEL_ROWS
GROUPS = [(dx, dc) for dx in range(NX) for dc in range(NC)]


def products_kernel(place, src, owner, target, count, left, *rest, halves):
    rights, rest = rest[: 1 + halves], rest[1 + halves:]
    outs, (packed, labels, spot_of, label_of, sem) = rest[: len(GROUPS)], rest[len(GROUPS):]
    front = pl.program_id(0)

    @pl.when(front == 0)
    def _():
        x, z, core = place[0], place[1], place[2]
        live = count[0]

        def clear(i, carry):
            label_of[i] = -1
            return carry

        lax.fori_loop(0, SPOTS + 1, clear, 0)

        def put(s, carry):
            o = owner[s]
            dx = (o // (NZ * NC) - x + NX) % NX
            dz = ((o // NC) % NZ - z + NZ) % NZ
            dc = (o % NC - core + NC) % NC
            spot = jnp.where(s < live, (dx * NC + dc) * NZ + dz, SPOTS)
            spot_of[src[s]] = spot
            label_of[spot] = target[s]
            return carry

        lax.fori_loop(0, SLOTS, put, 0)
        packed[...] = jnp.zeros_like(packed)
        row = lax.broadcasted_iota(jnp.int32, (LABEL_ROWS, COLS), 0)
        for g in range(len(GROUPS)):
            tile = jnp.full((LABEL_ROWS, COLS), -1, jnp.int32)
            for dz in range(NZ):
                tile = jnp.where(row == dz, label_of[g * NZ + dz], tile)
            labels[g * LABEL_ROWS:(g + 1) * LABEL_ROWS, :] = tile.astype(jnp.float32).astype(jnp.bfloat16)

    for b in range(BLOCKS):
        parts = [r[0, b] for r in rights]
        right = parts[0] if len(parts) == 1 else jnp.concatenate(parts, axis=0)
        mine = left[0, b:].reshape((BLOCKS - b) * ROWS, WIDTH)
        product = lax.dot_general(
            mine, right, (((1,), (1,)), ((), ())), preferred_element_type=jnp.float32
        ).astype(jnp.bfloat16)
        for a in range(b, BLOCKS):
            spot = spot_of[front * PAIRS + a * (a + 1) // 2 + b]
            packed[pl.ds(pl.multiple_of(spot * ROWS, ROWS), ROWS), :] = product[(a - b) * ROWS:(a - b + 1) * ROWS]

    @pl.when(front == FRONTS - 1)
    def _():
        copies = []
        for g, out in enumerate(outs):
            copies.append(pltpu.make_async_copy(
                packed.at[pl.ds(g * NZ * ROWS, NZ * ROWS)], out.at[pl.ds(0, NZ * ROWS)], sem.at[2 * g]))
            copies.append(pltpu.make_async_copy(
                labels.at[pl.ds(g * LABEL_ROWS, LABEL_ROWS)], out.at[pl.ds(NZ * ROWS, LABEL_ROWS)],
                sem.at[2 * g + 1]))
        for c in copies:
            c.start()
        for c in copies:
            c.wait()


def products(place, src, owner, target, count, left, rights):
    smem = pl.BlockSpec(memory_space=pltpu.SMEM)
    by_front = lambda rows: pl.BlockSpec((1, BLOCKS, rows, WIDTH), lambda f: (f, 0, 0, 0))
    return pl.pallas_call(
        functools.partial(products_kernel, halves=len(rights) - 1),
        grid=(FRONTS,),
        in_specs=[smem] * 5 + [by_front(ROWS)] + [by_front(r.shape[2]) for r in rights],
        out_specs=[pl.BlockSpec(memory_space=pl.ANY)] * len(GROUPS),
        out_shape=[jax.ShapeDtypeStruct((SENT_ROWS, COLS), jnp.bfloat16)] * len(GROUPS),
        scratch_shapes=[
            pltpu.VMEM(((SPOTS + 1) * ROWS, COLS), jnp.bfloat16),
            pltpu.VMEM((len(GROUPS) * LABEL_ROWS, COLS), jnp.bfloat16),
            pltpu.SMEM((SLOTS,), jnp.int32),
            pltpu.SMEM((SPOTS + 1,), jnp.int32),
            pltpu.SemaphoreType.DMA((2 * len(GROUPS),)),
        ],
        compiler_params=pltpu.CompilerParams(
            dimension_semantics=("arbitrary",), vmem_limit_bytes=16 * 1024 * 1024),
        cost_estimate=pl.CostEstimate(
            flops=2 * SLOTS * ROWS * COLS * WIDTH, bytes_accessed=6 * 1024 * 1024, transcendentals=0),
        name="products",
    )(place, src, owner, target, count, left, *rights)


def combine_kernel(*refs):
    arrived, outs = refs[: len(GROUPS)], refs[len(GROUPS):]
    step = 32
    tags = [a[NZ * ROWS:SENT_ROWS, :].astype(jnp.float32) for a in arrived]
    for dz in range(NZ):
        tag = [jnp.broadcast_to(t[dz:dz + 1, :], (step, COLS)) for t in tags]

        def rows_of(r, carry, dz=dz, tag=tag):
            base = pl.multiple_of(r * step, step)
            sums = [jnp.zeros((step, COLS), jnp.float32) for _ in range(TARGETS)]
            for g in range(len(GROUPS)):
                v = arrived[g][pl.ds(dz * ROWS + base, step), :].astype(jnp.float32)
                for t in range(TARGETS):
                    sums[t] = sums[t] + jnp.where(tag[g] == float(t), v, 0.0)
            for t in range(TARGETS):
                outs[dz][pl.ds(t * ROWS + base, step), :] = sums[t].astype(jnp.bfloat16)
            return carry

        lax.fori_loop(0, ROWS // step, rows_of, 0)


def combine(arrived):
    whole = pl.BlockSpec(memory_space=pltpu.VMEM)
    return pl.pallas_call(
        combine_kernel,
        in_specs=[whole] * len(GROUPS),
        out_specs=[whole] * NZ,
        out_shape=[jax.ShapeDtypeStruct((TARGETS * ROWS, COLS), jnp.bfloat16)] * NZ,
        compiler_params=pltpu.CompilerParams(vmem_limit_bytes=16 * 1024 * 1024),
        cost_estimate=pl.CostEstimate(
            flops=8 * SPOTS * ROWS * COLS, bytes_accessed=3 * 1024 * 1024, transcendentals=0),
        name="combine",
    )(*arrived)


def finish_kernel(piece, parent, *refs):
    first, plus, minus, last = (refs[NZ * k:NZ * (k + 1)] for k in range(4))
    out = refs[4 * NZ]
    me = piece[0]
    half = COLS // 2

    def total(group):
        s = group[0][...].astype(jnp.float32)
        for g in group[1:]:
            s = s + g[...].astype(jnp.float32)
        return s

    own, low, high, far = total(first), total(plus), total(minus), total(last)
    for d, value in (
        (0, own),
        (1, jnp.concatenate([low[:, :half], high[:, :half]], axis=1)),
        (3, jnp.concatenate([low[:, half:], high[:, half:]], axis=1)),
        (2, far),
    ):
        cols = pl.ds(pl.multiple_of(((me + d) % NY) * COLS, COLS), COLS)
        out[0, :, cols] = parent[0, :, cols] - value


def finish(piece, parent, chunks):
    by_target = pl.BlockSpec((ROWS, COLS), lambda t: (t, 0))
    wide = pl.BlockSpec((1, ROWS, NY * COLS), lambda t: (t, 0, 0))
    flat = [a for chunk in chunks for a in chunk]
    return pl.pallas_call(
        finish_kernel,
        grid=(TARGETS,),
        in_specs=[pl.BlockSpec(memory_space=pltpu.SMEM), wide] + [by_target] * len(flat),
        out_specs=wide,
        out_shape=jax.ShapeDtypeStruct(parent.shape, parent.dtype),
        compiler_params=pltpu.CompilerParams(
            dimension_semantics=("arbitrary",), vmem_limit_bytes=16 * 1024 * 1024),
        cost_estimate=pl.CostEstimate(
            flops=40 * TARGETS * ROWS * COLS, bytes_accessed=6 * 1024 * 1024, transcendentals=0),
        name="finish",
    )(piece, parent, *flat)


def over_y(v, d):
    return lax.ppermute(v, "grp", [(i, (i + d) % NY) for i in range(NY)])


def over_x(v, dx, dc):
    pairs = [(x * NC + c, (x + dx) % NX * NC + (c + dc) % NC) for x in range(NX) for c in range(NC)]
    return lax.ppermute(v, ("x", "core"), pairs)


def over_z(v, d):
    return lax.ppermute(v, "z", [(i, (i + d) % NZ) for i in range(NZ)])


def per_device(panels, parent, src_block, dest_owner, target, counts):
    place = jnp.stack([lax.axis_index("x"), lax.axis_index("z"), lax.axis_index("core")]).astype(jnp.int32)
    piece = lax.axis_index("grp").astype(jnp.int32).reshape(1)
    slots = (place, src_block[0], dest_owner[:, 0], target, counts)
    half = ROWS // 2
    lower, upper = panels[:, :, :half], panels[:, :, half:]
    rights = [(panels,)]
    rights.append((over_y(lower, -1), over_y(lower, 1)))
    rights.append((over_y(upper, -1), over_y(upper, 1)))
    rights.append((over_y(panels, 2),))
    summed = []
    for right in rights:
        packed = products(*slots, panels, right)
        arrived = [v if g == (0, 0) else over_x(v, *g) for g, v in zip(GROUPS, packed)]
        partial = combine(arrived)
        summed.append([v if d == 0 else over_z(v, d) for d, v in enumerate(partial)])
    return finish(piece, parent, summed)


def solution(mesh):
    split = Mesh(mesh.devices.reshape(NY, NX, NZ, NC), ("grp", "x", "z", "core"))
    col = ("x", "z", "core")
    placed = (
        P(col, None, "grp", None),
        P(col, "grp", None),
        P(col, None),
        P(col, None),
        P(col),
        P(col),
    )
    return jax.shard_map(
        per_device, mesh=split, in_specs=placed, out_specs=P(col, "grp", None), check_vma=False
    )
```

```python
import functools

import jax
import jax.numpy as jnp
from jax import lax
from jax.experimental import pallas as pl
from jax.experimental.pallas import tpu as pltpu
from jax.sharding import Mesh, PartitionSpec as P


NX, NZ, NC, NY = 4, 8, 2, 4
FRONTS, BLOCKS, ROWS, WIDTH = 4, 4, 128, 512
PAIRS, SLOTS, TARGETS = 10, 40, 4
COLS = 128
SPOTS = NX * NC * NZ
LABEL_ROWS = 16
SENT_ROWS = NZ * ROWS + LABEL_ROWS
GROUPS = [(dx, dc) for dx in range(NX) for dc in range(NC)]


def products_kernel(place, src, owner, target, count, left, *rest, parts):
    rights, outs, (made, pair_at, label_at) = rest[:parts], rest[parts:parts + len(GROUPS)], rest[-3:]
    x, z, core = place[0], place[1], place[2]
    live = count[0]

    def clear(i, carry):
        pair_at[i] = SLOTS
        label_at[i] = -1
        return carry

    lax.fori_loop(0, SPOTS + 1, clear, 0)

    def put(s, carry):
        o = owner[s]
        dx = (o // (NZ * NC) - x + NX) % NX
        dz = ((o // NC) % NZ - z + NZ) % NZ
        dc = (o % NC - core + NC) % NC
        spot = jnp.where(s < live, (dx * NC + dc) * NZ + dz, SPOTS)
        pair_at[spot] = src[s]
        label_at[spot] = target[s]
        return carry

    lax.fori_loop(0, SLOTS, put, 0)

    def piece(f, b):
        if parts == 0:
            return left[f, b]
        return jnp.concatenate([r[f, b] for r in rights], axis=0)

    def front(f, carry):
        for b in range(0, BLOCKS, 2):
            mine = left[f, b:].reshape((BLOCKS - b) * ROWS, WIDTH)
            right = jnp.concatenate([piece(f, b), piece(f, b + 1)], axis=0)
            product = lax.dot_general(
                mine, right, (((1,), (1,)), ((), ())), preferred_element_type=jnp.float32
            ).astype(jnp.bfloat16)
            for c in (b, b + 1):
                for a in range(c, BLOCKS):
                    at = pl.multiple_of((f * PAIRS + a * (a + 1) // 2 + c) * ROWS, ROWS)
                    made[pl.ds(at, ROWS), :] = product[(a - b) * ROWS:(a - b + 1) * ROWS, (c - b) * COLS:(c - b + 1) * COLS]
        return carry

    lax.fori_loop(0, FRONTS, front, 0)
    made[SLOTS * ROWS:, :] = jnp.zeros((ROWS, COLS), jnp.bfloat16)
    row = lax.broadcasted_iota(jnp.int32, (LABEL_ROWS, COLS), 0)
    for g, out in enumerate(outs):
        tile = jnp.full((LABEL_ROWS, COLS), -1, jnp.int32)
        for dz in range(NZ):
            tile = jnp.where(row == dz, label_at[g * NZ + dz], tile)
        out[NZ * ROWS:, :] = tile.astype(jnp.float32).astype(jnp.bfloat16)

        def place_block(dz, carry, g=g, out=out):
            at = pl.multiple_of(pair_at[g * NZ + dz] * ROWS, ROWS)
            out[pl.ds(pl.multiple_of(dz * ROWS, ROWS), ROWS), :] = made[pl.ds(at, ROWS), :]
            return carry

        lax.fori_loop(0, NZ, place_block, 0)


def products(place, src, owner, target, count, left, rights):
    smem = pl.BlockSpec(memory_space=pltpu.SMEM)
    whole = pl.BlockSpec(memory_space=pltpu.VMEM)
    parts = len(rights)
    return pl.pallas_call(
        functools.partial(products_kernel, parts=parts),
        in_specs=[smem] * 5 + [whole] * (1 + parts),
        out_specs=[whole] * len(GROUPS),
        out_shape=[jax.ShapeDtypeStruct((SENT_ROWS, COLS), jnp.bfloat16)] * len(GROUPS),
        scratch_shapes=[
            pltpu.VMEM(((SLOTS + 1) * ROWS, COLS), jnp.bfloat16),
            pltpu.SMEM((SPOTS + 1,), jnp.int32),
            pltpu.SMEM((SPOTS + 1,), jnp.int32),
        ],
        compiler_params=pltpu.CompilerParams(vmem_limit_bytes=16 * 1024 * 1024),
        cost_estimate=pl.CostEstimate(
            flops=2 * SLOTS * ROWS * COLS * WIDTH, bytes_accessed=6 * 1024 * 1024, transcendentals=0),
        name="products",
    )(place, src, owner, target, count, left, *rights)


def combine_kernel(place, *refs, packed):
    arrived, outs = refs[: len(GROUPS)], refs[len(GROUPS):]
    step = 32
    z = place[1]
    tags = [a[NZ * ROWS:SENT_ROWS, :].astype(jnp.float32) for a in arrived]
    for dz in range(NZ):
        tag = [jnp.broadcast_to(t[dz:dz + 1, :], (step, COLS)) for t in tags]
        out, start = (outs[0], (z + dz) % NZ * TARGETS * ROWS) if packed else (outs[dz], 0)

        def rows_of(r, carry, dz=dz, tag=tag, out=out, start=start):
            base = pl.multiple_of(r * step, step)
            sums = [jnp.zeros((step, COLS), jnp.float32) for _ in range(TARGETS)]
            for g in range(len(GROUPS)):
                v = arrived[g][pl.ds(dz * ROWS + base, step), :].astype(jnp.float32)
                for t in range(TARGETS):
                    sums[t] = sums[t] + jnp.where(tag[g] == float(t), v, 0.0)
            for t in range(TARGETS):
                at = pl.multiple_of(start + t * ROWS + base, step)
                out[pl.ds(at, step), :] = sums[t].astype(jnp.bfloat16)
            return carry

        lax.fori_loop(0, ROWS // step, rows_of, 0)


def combine(place, arrived, packed):
    whole = pl.BlockSpec(memory_space=pltpu.VMEM)
    rows = TARGETS * ROWS
    outs = [jax.ShapeDtypeStruct((NZ * rows, COLS), jnp.bfloat16)] if packed else [
        jax.ShapeDtypeStruct((rows, COLS), jnp.bfloat16)] * NZ
    return pl.pallas_call(
        functools.partial(combine_kernel, packed=packed),
        in_specs=[pl.BlockSpec(memory_space=pltpu.SMEM)] + [whole] * len(GROUPS),
        out_specs=[whole] * len(outs),
        out_shape=outs,
        compiler_params=pltpu.CompilerParams(vmem_limit_bytes=16 * 1024 * 1024),
        cost_estimate=pl.CostEstimate(
            flops=8 * SPOTS * ROWS * COLS, bytes_accessed=3 * 1024 * 1024, transcendentals=0),
        name="combine",
    )(place, *arrived)


def block_sum(parts):
    total = parts[0][...].astype(jnp.float32)
    for p in parts[1:]:
        total = total + p[...].astype(jnp.float32)
    return total


def finish_kernel(piece, parent, *refs, sizes):
    out = refs[-1]
    sums, at = [], 0
    for n in sizes:
        sums.append(block_sum(refs[at:at + n]))
        at += n
    own, low, high = sums
    me, half = piece[0], COLS // 2
    values = {
        0: own,
        1: jnp.concatenate([low[:, :half], high[:, :half]], axis=1),
        2: None,
        3: jnp.concatenate([low[:, half:], high[:, half:]], axis=1),
    }
    for d, value in values.items():
        cols = pl.ds(pl.multiple_of(((me + d) % NY) * COLS, COLS), COLS)
        out[0, :, cols] = parent[0, :, cols] if value is None else parent[0, :, cols] - value


def finish(piece, parent, chunks):
    wide = pl.BlockSpec((1, ROWS, NY * COLS), lambda t: (t, 0, 0))
    flat, specs, sizes = [], [], []
    for chunk in chunks:
        if len(chunk) == 1:
            flat += [chunk[0]] * NZ
            specs += [pl.BlockSpec((ROWS, COLS), lambda t, z=z: (z * TARGETS + t, 0)) for z in range(NZ)]
        else:
            flat += chunk
            specs += [pl.BlockSpec((ROWS, COLS), lambda t: (t, 0))] * NZ
        sizes.append(NZ)
    return pl.pallas_call(
        functools.partial(finish_kernel, sizes=tuple(sizes)),
        grid=(TARGETS,),
        in_specs=[pl.BlockSpec(memory_space=pltpu.SMEM), wide] + specs,
        out_specs=wide,
        out_shape=jax.ShapeDtypeStruct(parent.shape, parent.dtype),
        compiler_params=pltpu.CompilerParams(
            dimension_semantics=("arbitrary",), vmem_limit_bytes=16 * 1024 * 1024),
        cost_estimate=pl.CostEstimate(
            flops=30 * TARGETS * ROWS * COLS, bytes_accessed=5 * 1024 * 1024, transcendentals=0),
        name="finish",
    )(piece, parent, *flat)


def finish_last_kernel(piece, sofar, *refs):
    parts, (out, held, sem) = refs[:NZ], refs[NZ:]
    cols = pl.ds(pl.multiple_of((piece[0] + 2) % NY * COLS, COLS), COLS)
    load = pltpu.make_async_copy(sofar.at[:, :, cols], held, sem.at[0])
    load.start()
    load.wait()
    stores = []
    for t in range(TARGETS):
        held[t] = held[t] - block_sum([p.at[pl.ds(t * ROWS, ROWS)] for p in parts])
        stores.append(pltpu.make_async_copy(held.at[t], out.at[t, :, cols], sem.at[1 + t]))
        stores[-1].start()
    for c in stores:
        c.wait()


def finish_last(piece, sofar, chunk):
    hbm = pl.BlockSpec(memory_space=pl.ANY)
    return pl.pallas_call(
        finish_last_kernel,
        in_specs=[pl.BlockSpec(memory_space=pltpu.SMEM), hbm] + [pl.BlockSpec(memory_space=pltpu.VMEM)] * NZ,
        out_specs=hbm,
        out_shape=jax.ShapeDtypeStruct(sofar.shape, sofar.dtype),
        scratch_shapes=[
            pltpu.VMEM((TARGETS, ROWS, COLS), jnp.float32),
            pltpu.SemaphoreType.DMA((1 + TARGETS,)),
        ],
        input_output_aliases={1: 0},
        compiler_params=pltpu.CompilerParams(vmem_limit_bytes=8 * 1024 * 1024),
        cost_estimate=pl.CostEstimate(
            flops=10 * TARGETS * ROWS * COLS, bytes_accessed=2 * 1024 * 1024, transcendentals=0),
        name="finish_last",
    )(piece, sofar, *chunk)


def over_y(v, d):
    return lax.ppermute(v, "grp", [(i, (i + d) % NY) for i in range(NY)])


def over_x(v, dx, dc):
    pairs = [(x * NC + c, (x + dx) % NX * NC + (c + dc) % NC) for x in range(NX) for c in range(NC)]
    return lax.ppermute(v, ("x", "core"), pairs)


def over_z(v, d):
    return lax.ppermute(v, "z", [(i, (i + d) % NZ) for i in range(NZ)])


def per_device(panels, parent, src_block, dest_owner, target, counts):
    place = jnp.stack([lax.axis_index("x"), lax.axis_index("z"), lax.axis_index("core")]).astype(jnp.int32)
    piece = lax.axis_index("grp").astype(jnp.int32).reshape(1)
    slots = (place, src_block[0], dest_owner[:, 0], target, counts)
    half = ROWS // 2
    lower = panels[:, :, :half]
    upper = lax.optimization_barrier(panels)[:, :, half:]
    low_next, low_prev = over_y(lower, -1), over_y(lower, 1)
    up_next, up_prev = over_y(upper, -1), over_y(upper, 1)
    low_far = over_y(low_next, -1)
    up_far = over_y(up_prev, 1)
    rights = [(), (low_next, low_prev), (up_next, up_prev), (low_far, up_far)]
    summed = []
    for k, right in enumerate(rights):
        packed = products(*slots, panels, right)
        arrived = [v if g == (0, 0) else over_x(v, *g) for g, v in zip(GROUPS, packed)]
        partial = combine(place, arrived, k in (0, 2))
        if k in (0, 2):
            summed.append([lax.all_to_all(partial[0], "z", 0, 0, tiled=True)])
        else:
            summed.append([v if d == 0 else over_z(v, d) for d, v in enumerate(partial)])
    sofar = finish(piece, parent, summed[:3])
    return finish_last(piece, sofar, summed[3])


def solution(mesh):
    split = Mesh(mesh.devices.reshape(NY, NX, NZ, NC), ("grp", "x", "z", "core"))
    col = ("x", "z", "core")
    placed = (
        P(col, None, "grp", None),
        P(col, "grp", None),
        P(col, None),
        P(col, None),
        P(col),
        P(col),
    )
    return jax.shard_map(
        per_device, mesh=split, in_specs=placed, out_specs=P(col, "grp", None), check_vma=False
    )
```

```python
import functools

import jax
import jax.numpy as jnp
from jax import lax
from jax.experimental import pallas as pl
from jax.experimental.pallas import tpu as pltpu
from jax.sharding import Mesh, PartitionSpec as P


NX, NZ, NC, NY = 4, 8, 2, 4
FRONTS, BLOCKS, ROWS, WIDTH = 4, 4, 128, 512
PAIRS, SLOTS, TARGETS = 10, 40, 4
COLS = 128
SPOTS = NX * NC * NZ
LABEL_ROWS = 16
PER_X = NC * NZ
SENT_ROWS = PER_X * ROWS + LABEL_ROWS
VMEM = 12 * 1024 * 1024
SUM_ROWS = TARGETS * ROWS
HOPS = NZ // 2


def products_kernel(place, src, owner, target, count, left, *rest, parts):
    rights, outs, (made, pair_at, label_at) = rest[:parts], rest[parts:parts + NX], rest[-3:]
    x, z, core = place[0], place[1], place[2]
    live = count[0]

    def clear(i, carry):
        pair_at[i] = SLOTS
        label_at[i] = -1
        return carry

    lax.fori_loop(0, SPOTS + 1, clear, 0)

    def put(s, carry):
        o = owner[s]
        dx = (o // (NZ * NC) - x + NX) % NX
        dz = ((o // NC) % NZ - z + NZ) % NZ
        dc = (o % NC - core + NC) % NC
        spot = jnp.where(s < live, (dx * NC + dc) * NZ + dz, SPOTS)
        pair_at[spot] = src[s]
        label_at[spot] = target[s]
        return carry

    lax.fori_loop(0, SLOTS, put, 0)

    def piece(f, b):
        if parts == 0:
            return left[f, b]
        return jnp.concatenate([r[f, b] for r in rights], axis=0)

    def front(f, carry):
        for b in range(0, BLOCKS, 2):
            mine = left[f, b:].reshape((BLOCKS - b) * ROWS, WIDTH)
            right = jnp.concatenate([piece(f, b), piece(f, b + 1)], axis=0)
            product = lax.dot_general(
                mine, right, (((1,), (1,)), ((), ())), preferred_element_type=jnp.float32
            ).astype(jnp.bfloat16)
            for c in (b, b + 1):
                for a in range(c, BLOCKS):
                    at = pl.multiple_of((f * PAIRS + a * (a + 1) // 2 + c) * ROWS, ROWS)
                    made[pl.ds(at, ROWS), :] = product[(a - b) * ROWS:(a - b + 1) * ROWS, (c - b) * COLS:(c - b + 1) * COLS]
        return carry

    lax.fori_loop(0, FRONTS, front, 0)
    made[SLOTS * ROWS:, :] = jnp.zeros((ROWS, COLS), jnp.bfloat16)
    row = lax.broadcasted_iota(jnp.int32, (LABEL_ROWS, COLS), 0)
    for dx, out in enumerate(outs):
        tile = jnp.full((LABEL_ROWS, COLS), -1, jnp.int32)
        for i in range(PER_X):
            tile = jnp.where(row == i, label_at[dx * PER_X + i], tile)
        out[PER_X * ROWS:, :] = tile.astype(jnp.float32).astype(jnp.bfloat16)

        def place_block(i, carry, dx=dx, out=out):
            at = pl.multiple_of(pair_at[dx * PER_X + i] * ROWS, ROWS)
            out[pl.ds(pl.multiple_of(i * ROWS, ROWS), ROWS), :] = made[pl.ds(at, ROWS), :]
            return carry

        lax.fori_loop(0, PER_X, place_block, 0)


def products(place, src, owner, target, count, left, rights):
    smem = pl.BlockSpec(memory_space=pltpu.SMEM)
    whole = pl.BlockSpec(memory_space=pltpu.VMEM)
    parts = len(rights)
    return pl.pallas_call(
        functools.partial(products_kernel, parts=parts),
        in_specs=[smem] * 5 + [whole] * (1 + parts),
        out_specs=[whole] * NX,
        out_shape=[jax.ShapeDtypeStruct((SENT_ROWS, COLS), jnp.bfloat16)] * NX,
        scratch_shapes=[
            pltpu.VMEM(((SLOTS + 1) * ROWS, COLS), jnp.bfloat16),
            pltpu.SMEM((SPOTS + 1,), jnp.int32),
            pltpu.SMEM((SPOTS + 1,), jnp.int32),
        ],
        compiler_params=pltpu.CompilerParams(vmem_limit_bytes=VMEM),
        cost_estimate=pl.CostEstimate(
            flops=2 * SLOTS * ROWS * COLS * WIDTH, bytes_accessed=6 * 1024 * 1024, transcendentals=0),
        name="products",
    )(place, src, owner, target, count, left, *rights)


def first_move(dc, dz):
    if dz % 2 == 0:
        return 2 * dc, dz // 2
    return (1, dz // 2) if dc == 0 else (3, (dz + 1) // 2 % HOPS)


def combine_kernel(*refs):
    arrived, outs = refs[:NX], refs[NX:]
    step = 32
    tags = [a[PER_X * ROWS:SENT_ROWS, :].astype(jnp.float32) for a in arrived]
    for i in range(PER_X):
        tag = [jnp.broadcast_to(t[i:i + 1, :], (step, COLS)) for t in tags]
        way, left = first_move(i // NZ, i % NZ)

        def rows_of(r, carry, i=i, tag=tag, out=outs[way], start=left * SUM_ROWS):
            base = pl.multiple_of(r * step, step)
            sums = [jnp.zeros((step, COLS), jnp.float32) for _ in range(TARGETS)]
            for g in range(NX):
                v = arrived[g][pl.ds(i * ROWS + base, step), :].astype(jnp.float32)
                for t in range(TARGETS):
                    sums[t] = sums[t] + jnp.where(tag[g] == float(t), v, 0.0)
            for t in range(TARGETS):
                out[pl.ds(start + t * ROWS + base, step), :] = sums[t].astype(jnp.bfloat16)
            return carry

        lax.fori_loop(0, ROWS // step, rows_of, 0)


def combine(arrived):
    whole = pl.BlockSpec(memory_space=pltpu.VMEM)
    return pl.pallas_call(
        combine_kernel,
        in_specs=[whole] * NX,
        out_specs=[whole] * 4,
        out_shape=[jax.ShapeDtypeStruct((HOPS * SUM_ROWS, COLS), jnp.bfloat16)] * 4,
        compiler_params=pltpu.CompilerParams(vmem_limit_bytes=VMEM),
        cost_estimate=pl.CostEstimate(
            flops=8 * SPOTS * ROWS * COLS, bytes_accessed=4 * 1024 * 1024, transcendentals=0),
        name="combine",
    )(*arrived)


def merge_kernel(*refs):
    parts, outs = refs[:4], refs[4:]
    step = 64
    for h, out in enumerate(outs):

        def rows_of(r, carry, h=h, out=out):
            base = pl.multiple_of(r * step, step)
            total = [p[pl.ds(h * SUM_ROWS + base, step), :].astype(jnp.float32) for p in parts]
            out[pl.ds(base, step), :] = (total[0] + total[1] + (total[2] + total[3])).astype(jnp.bfloat16)
            return carry

        lax.fori_loop(0, SUM_ROWS // step, rows_of, 0)


def merge(parts):
    whole = pl.BlockSpec(memory_space=pltpu.VMEM)
    return pl.pallas_call(
        merge_kernel,
        in_specs=[whole] * 4,
        out_specs=[whole] * HOPS,
        out_shape=[jax.ShapeDtypeStruct((SUM_ROWS, COLS), jnp.bfloat16)] * HOPS,
        compiler_params=pltpu.CompilerParams(vmem_limit_bytes=VMEM),
        cost_estimate=pl.CostEstimate(
            flops=4 * HOPS * SUM_ROWS * COLS, bytes_accessed=2 * 1024 * 1024, transcendentals=0),
        name="merge",
    )(*parts)


def block_sum(parts):
    total = parts[0][...].astype(jnp.float32)
    for p in parts[1:]:
        total = total + p[...].astype(jnp.float32)
    return total


def finish_kernel(piece, parent, *refs, sizes):
    out = refs[-1]
    sums, at = [], 0
    for n in sizes:
        sums.append(block_sum(refs[at:at + n]))
        at += n
    own, low, high = sums
    me, half = piece[0], COLS // 2
    values = {
        0: own,
        1: jnp.concatenate([low[:, :half], high[:, :half]], axis=1),
        2: None,
        3: jnp.concatenate([low[:, half:], high[:, half:]], axis=1),
    }
    for d, value in values.items():
        cols = pl.ds(pl.multiple_of(((me + d) % NY) * COLS, COLS), COLS)
        out[0, :, cols] = parent[0, :, cols] if value is None else parent[0, :, cols] - value


def finish(piece, parent, chunks):
    wide = pl.BlockSpec((1, ROWS, NY * COLS), lambda t: (t, 0, 0))
    flat = [part for chunk in chunks for part in chunk]
    return pl.pallas_call(
        functools.partial(finish_kernel, sizes=tuple(len(chunk) for chunk in chunks)),
        grid=(TARGETS,),
        in_specs=[pl.BlockSpec(memory_space=pltpu.SMEM), wide]
        + [pl.BlockSpec((ROWS, COLS), lambda t: (t, 0))] * len(flat),
        out_specs=wide,
        out_shape=jax.ShapeDtypeStruct(parent.shape, parent.dtype),
        compiler_params=pltpu.CompilerParams(
            dimension_semantics=("arbitrary",), vmem_limit_bytes=VMEM),
        cost_estimate=pl.CostEstimate(
            flops=30 * TARGETS * ROWS * COLS, bytes_accessed=5 * 1024 * 1024, transcendentals=0),
        name="finish",
    )(piece, parent, *flat)


def finish_last_kernel(piece, sofar, *refs):
    parts, (out, held, sem) = refs[:HOPS], refs[HOPS:]
    cols = pl.ds(pl.multiple_of((piece[0] + 2) % NY * COLS, COLS), COLS)
    load = pltpu.make_async_copy(sofar.at[:, :, cols], held, sem.at[0])
    load.start()
    load.wait()
    stores = []
    for t in range(TARGETS):
        held[t] = held[t] - block_sum([p.at[pl.ds(t * ROWS, ROWS)] for p in parts])
        stores.append(pltpu.make_async_copy(held.at[t], out.at[t, :, cols], sem.at[1 + t]))
        stores[-1].start()
    for c in stores:
        c.wait()


def finish_last(piece, sofar, chunk):
    hbm = pl.BlockSpec(memory_space=pl.ANY)
    return pl.pallas_call(
        finish_last_kernel,
        in_specs=[pl.BlockSpec(memory_space=pltpu.SMEM), hbm] + [pl.BlockSpec(memory_space=pltpu.VMEM)] * HOPS,
        out_specs=hbm,
        out_shape=jax.ShapeDtypeStruct(sofar.shape, sofar.dtype),
        scratch_shapes=[
            pltpu.VMEM((TARGETS, ROWS, COLS), jnp.float32),
            pltpu.SemaphoreType.DMA((1 + TARGETS,)),
        ],
        input_output_aliases={1: 0},
        compiler_params=pltpu.CompilerParams(vmem_limit_bytes=VMEM),
        cost_estimate=pl.CostEstimate(
            flops=10 * TARGETS * ROWS * COLS, bytes_accessed=2 * 1024 * 1024, transcendentals=0),
        name="finish_last",
    )(piece, sofar, *chunk)


def over_y(v, d):
    return lax.ppermute(v, "grp", [(i, (i + d) % NY) for i in range(NY)])


def over_x(v, dx):
    return lax.ppermute(v, "x", [(i, (i + dx) % NX) for i in range(NX)])


def over_z(v, dz, dc):
    pairs = [(z * NC + c, (z + dz) % NZ * NC + (c + dc) % NC) for z in range(NZ) for c in range(NC)]
    return lax.ppermute(v, ("z", "core"), pairs)


def per_device(panels, parent, src_block, dest_owner, target, counts):
    place = jnp.stack([lax.axis_index("x"), lax.axis_index("z"), lax.axis_index("core")]).astype(jnp.int32)
    piece = lax.axis_index("grp").astype(jnp.int32).reshape(1)
    slots = (place, src_block[0], dest_owner[:, 0], target, counts)
    half = ROWS // 2
    lower = panels[:, :, :half]
    upper = lax.optimization_barrier(panels)[:, :, half:]
    low_next, low_prev = over_y(lower, -1), over_y(lower, 1)
    up_next, up_prev = over_y(upper, -1), over_y(upper, 1)
    low_far = over_y(low_next, -1)
    up_far = over_y(up_prev, 1)
    rights = [(), (low_next, low_prev), (up_next, up_prev), (low_far, up_far)]
    summed = []
    for right in rights:
        packed = products(*slots, panels, right)
        arrived = [packed[0]] + [over_x(packed[d], d) for d in range(1, NX)]
        keep, plus, swap, cross = combine(arrived)
        parts = [keep, over_z(plus, 1, 0), over_z(swap, 0, 1), over_z(cross, -1, 1)]
        merged = merge(parts)
        summed.append([merged[0]] + [over_z(merged[h], 2 * h, 0) for h in range(1, HOPS)])
    sofar = finish(piece, parent, summed[:3])
    return finish_last(piece, sofar, summed[3])


def solution(mesh):
    split = Mesh(mesh.devices.reshape(NY, NX, NZ, NC), ("grp", "x", "z", "core"))
    col = ("x", "z", "core")
    placed = (
        P(col, None, "grp", None),
        P(col, "grp", None),
        P(col, None),
        P(col, None),
        P(col),
        P(col),
    )
    return jax.shard_map(
        per_device, mesh=split, in_specs=placed, out_specs=P(col, "grp", None), check_vma=False
    )
```

```python
import functools

import jax
import jax.numpy as jnp
from jax import lax
from jax.experimental import pallas as pl
from jax.experimental.pallas import tpu as pltpu
from jax.sharding import Mesh, PartitionSpec as P


NX, NZ, NC, NY = 4, 8, 2, 4
FRONTS, BLOCKS, ROWS, WIDTH = 4, 4, 128, 512
PAIRS, SLOTS, TARGETS = 10, 40, 4
COLS = 128
SPOTS = NX * NC * NZ
LABEL_ROWS = 16
PER_X = NC * NZ
SENT_ROWS = PER_X * ROWS + LABEL_ROWS
VMEM = 12 * 1024 * 1024
SUM_ROWS = TARGETS * ROWS
HOPS = NZ // 2


def products_kernel(place, src, owner, target, count, left, *rest, parts):
    rights, outs, (made, pair_at, label_at) = rest[:parts], rest[parts:parts + NX], rest[-3:]
    x, z, core = place[0], place[1], place[2]
    live = count[0]

    def clear(i, carry):
        pair_at[i] = SLOTS
        label_at[i] = -1
        return carry

    lax.fori_loop(0, SPOTS + 1, clear, 0)

    def put(s, carry):
        o = owner[s]
        dx = (o // (NZ * NC) - x + NX) % NX
        dz = ((o // NC) % NZ - z + NZ) % NZ
        dc = (o % NC - core + NC) % NC
        spot = jnp.where(s < live, (dx * NC + dc) * NZ + dz, SPOTS)
        pair_at[spot] = src[s]
        label_at[spot] = target[s]
        return carry

    lax.fori_loop(0, SLOTS, put, 0)

    def piece(f, b):
        if parts == 0:
            return left[f, b]
        return jnp.concatenate([r[f, b] for r in rights], axis=0)

    def front(f, carry):
        for b in range(0, BLOCKS, 2):
            mine = left[f, b:].reshape((BLOCKS - b) * ROWS, WIDTH)
            right = jnp.concatenate([piece(f, b), piece(f, b + 1)], axis=0)
            product = lax.dot_general(
                mine, right, (((1,), (1,)), ((), ())), preferred_element_type=jnp.float32
            ).astype(jnp.bfloat16)
            for c in (b, b + 1):
                for a in range(c, BLOCKS):
                    at = pl.multiple_of((f * PAIRS + a * (a + 1) // 2 + c) * ROWS, ROWS)
                    made[pl.ds(at, ROWS), :] = product[(a - b) * ROWS:(a - b + 1) * ROWS, (c - b) * COLS:(c - b + 1) * COLS]
        return carry

    lax.fori_loop(0, FRONTS, front, 0)
    made[SLOTS * ROWS:, :] = jnp.zeros((ROWS, COLS), jnp.bfloat16)
    row = lax.broadcasted_iota(jnp.int32, (LABEL_ROWS, COLS), 0)
    for dx, out in enumerate(outs):
        tile = jnp.full((LABEL_ROWS, COLS), -1, jnp.int32)
        for i in range(PER_X):
            tile = jnp.where(row == i, label_at[dx * PER_X + i], tile)
        out[PER_X * ROWS:, :] = tile.astype(jnp.float32).astype(jnp.bfloat16)

        def place_block(i, carry, dx=dx, out=out):
            at = pl.multiple_of(pair_at[dx * PER_X + i] * ROWS, ROWS)
            out[pl.ds(pl.multiple_of(i * ROWS, ROWS), ROWS), :] = made[pl.ds(at, ROWS), :]
            return carry

        lax.fori_loop(0, PER_X, place_block, 0)


def products(place, src, owner, target, count, left, rights):
    smem = pl.BlockSpec(memory_space=pltpu.SMEM)
    whole = pl.BlockSpec(memory_space=pltpu.VMEM)
    parts = len(rights)
    return pl.pallas_call(
        functools.partial(products_kernel, parts=parts),
        in_specs=[smem] * 5 + [whole] * (1 + parts),
        out_specs=[whole] * NX,
        out_shape=[jax.ShapeDtypeStruct((SENT_ROWS, COLS), jnp.bfloat16)] * NX,
        scratch_shapes=[
            pltpu.VMEM(((SLOTS + 1) * ROWS, COLS), jnp.bfloat16),
            pltpu.SMEM((SPOTS + 1,), jnp.int32),
            pltpu.SMEM((SPOTS + 1,), jnp.int32),
        ],
        compiler_params=pltpu.CompilerParams(vmem_limit_bytes=VMEM),
        cost_estimate=pl.CostEstimate(
            flops=2 * SLOTS * ROWS * COLS * WIDTH, bytes_accessed=6 * 1024 * 1024, transcendentals=0),
        name="products",
    )(place, src, owner, target, count, left, *rights)


def combine_kernel(*refs):
    arrived, outs = refs[:NX], refs[NX:]
    step = 32
    tags = [a[PER_X * ROWS:SENT_ROWS, :].astype(jnp.float32) for a in arrived]
    for i in range(PER_X):
        tag = [jnp.broadcast_to(t[i:i + 1, :], (step, COLS)) for t in tags]

        def rows_of(r, carry, i=i, tag=tag, out=outs[i // NZ], start=i % NZ * SUM_ROWS):
            base = pl.multiple_of(r * step, step)
            sums = [jnp.zeros((step, COLS), jnp.float32) for _ in range(TARGETS)]
            for g in range(NX):
                v = arrived[g][pl.ds(i * ROWS + base, step), :].astype(jnp.float32)
                for t in range(TARGETS):
                    sums[t] = sums[t] + jnp.where(tag[g] == float(t), v, 0.0)
            for t in range(TARGETS):
                out[pl.ds(start + t * ROWS + base, step), :] = sums[t].astype(out.dtype)
            return carry

        lax.fori_loop(0, ROWS // step, rows_of, 0)


def in_vmem(kernel, inputs, shapes):
    whole = pl.BlockSpec(memory_space=pltpu.VMEM)
    return pl.pallas_call(
        kernel,
        in_specs=[whole] * len(inputs),
        out_specs=[whole] * len(shapes),
        out_shape=[jax.ShapeDtypeStruct((rows, COLS), dtype) for rows, dtype in shapes],
        compiler_params=pltpu.CompilerParams(vmem_limit_bytes=VMEM),
        cost_estimate=pl.CostEstimate(
            flops=8 * SPOTS * ROWS * COLS, bytes_accessed=3 * 1024 * 1024, transcendentals=0),
    )(*inputs)


def combine(arrived):
    rows = NZ * SUM_ROWS
    return in_vmem(combine_kernel, arrived, [(rows, jnp.float32), (rows, jnp.bfloat16)])


def split_kernel(keep, swapped, even, up, down):
    step = 64
    half = SUM_ROWS // 2

    def add(out, at, start, count):
        def rows_of(r, carry):
            base = pl.multiple_of(r * step, step)
            total = keep[pl.ds(start + base, step), :] + swapped[pl.ds(start + base, step), :].astype(jnp.float32)
            out[pl.ds(at + base, step), :] = total.astype(out.dtype)
            return carry

        lax.fori_loop(0, count // step, rows_of, 0)

    for dz in range(NZ):
        if dz % 2 == 0:
            add(even, dz // 2 * SUM_ROWS, dz * SUM_ROWS, SUM_ROWS)
        else:
            add(up, dz // 2 * half, dz * SUM_ROWS, half)
            add(down, (dz + 1) // 2 % HOPS * half, dz * SUM_ROWS + half, half)


def split(keep, swapped):
    rows = HOPS * SUM_ROWS
    return in_vmem(
        split_kernel, (keep, swapped),
        [(rows, jnp.float32), (rows // 2, jnp.bfloat16), (rows // 2, jnp.bfloat16)])


def merge_kernel(even, up, down, *outs):
    step = 64
    half = SUM_ROWS // 2
    for h, out in enumerate(outs):
        for part, moved in enumerate((up, down)):

            def rows_of(r, carry, h=h, out=out, part=part, moved=moved):
                base = pl.multiple_of(r * step, step)
                total = even[pl.ds(h * SUM_ROWS + part * half + base, step), :] + moved[
                    pl.ds(h * half + base, step), :].astype(jnp.float32)
                out[pl.ds(part * half + base, step), :] = total.astype(out.dtype)
                return carry

            lax.fori_loop(0, half // step, rows_of, 0)


def merge(parts):
    return in_vmem(
        merge_kernel, parts,
        [(SUM_ROWS, jnp.float32)] + [(SUM_ROWS, jnp.bfloat16)] * (HOPS - 1))


def block_sum(parts):
    total = parts[0][...].astype(jnp.float32)
    for p in parts[1:]:
        total = total + p[...].astype(jnp.float32)
    return total


def finish_kernel(piece, parent, *refs, sizes):
    out = refs[-1]
    sums, at = [], 0
    for n in sizes:
        sums.append(block_sum(refs[at:at + n]))
        at += n
    own, low, high = sums
    me, half = piece[0], COLS // 2
    values = {
        0: own,
        1: jnp.concatenate([low[:, :half], high[:, :half]], axis=1),
        2: None,
        3: jnp.concatenate([low[:, half:], high[:, half:]], axis=1),
    }
    for d, value in values.items():
        cols = pl.ds(pl.multiple_of(((me + d) % NY) * COLS, COLS), COLS)
        out[0, :, cols] = parent[0, :, cols] if value is None else parent[0, :, cols] - value


def finish(piece, parent, chunks):
    wide = pl.BlockSpec((1, ROWS, NY * COLS), lambda t: (t, 0, 0))
    flat = [part for chunk in chunks for part in chunk]
    return pl.pallas_call(
        functools.partial(finish_kernel, sizes=tuple(len(chunk) for chunk in chunks)),
        grid=(TARGETS,),
        in_specs=[pl.BlockSpec(memory_space=pltpu.SMEM), wide]
        + [pl.BlockSpec((ROWS, COLS), lambda t: (t, 0))] * len(flat),
        out_specs=wide,
        out_shape=jax.ShapeDtypeStruct(parent.shape, parent.dtype),
        compiler_params=pltpu.CompilerParams(
            dimension_semantics=("arbitrary",), vmem_limit_bytes=VMEM),
        cost_estimate=pl.CostEstimate(
            flops=30 * TARGETS * ROWS * COLS, bytes_accessed=5 * 1024 * 1024, transcendentals=0),
        name="finish",
    )(piece, parent, *flat)


def finish_last_kernel(piece, sofar, *refs):
    parts, (out, held, sem) = refs[:HOPS], refs[HOPS:]
    cols = pl.ds(pl.multiple_of((piece[0] + 2) % NY * COLS, COLS), COLS)
    load = pltpu.make_async_copy(sofar.at[:, :, cols], held, sem.at[0])
    load.start()
    load.wait()
    stores = []
    for t in range(TARGETS):
        held[t] = held[t] - block_sum([p.at[pl.ds(t * ROWS, ROWS)] for p in parts])
        stores.append(pltpu.make_async_copy(held.at[t], out.at[t, :, cols], sem.at[1 + t]))
        stores[-1].start()
    for c in stores:
        c.wait()


def finish_last(piece, sofar, chunk):
    hbm = pl.BlockSpec(memory_space=pl.ANY)
    return pl.pallas_call(
        finish_last_kernel,
        in_specs=[pl.BlockSpec(memory_space=pltpu.SMEM), hbm] + [pl.BlockSpec(memory_space=pltpu.VMEM)] * HOPS,
        out_specs=hbm,
        out_shape=jax.ShapeDtypeStruct(sofar.shape, sofar.dtype),
        scratch_shapes=[
            pltpu.VMEM((TARGETS, ROWS, COLS), jnp.float32),
            pltpu.SemaphoreType.DMA((1 + TARGETS,)),
        ],
        input_output_aliases={1: 0},
        compiler_params=pltpu.CompilerParams(vmem_limit_bytes=VMEM),
        cost_estimate=pl.CostEstimate(
            flops=10 * TARGETS * ROWS * COLS, bytes_accessed=2 * 1024 * 1024, transcendentals=0),
        name="finish_last",
    )(piece, sofar, *chunk)


def over_y(v, d):
    return lax.ppermute(v, "grp", [(i, (i + d) % NY) for i in range(NY)])


def over_x(v, dx):
    return lax.ppermute(v, "x", [(i, (i + dx) % NX) for i in range(NX)])


def over_z(v, dz, dc):
    pairs = [(z * NC + c, (z + dz) % NZ * NC + (c + dc) % NC) for z in range(NZ) for c in range(NC)]
    return lax.ppermute(v, ("z", "core"), pairs)


def per_device(panels, parent, src_block, dest_owner, target, counts):
    place = jnp.stack([lax.axis_index("x"), lax.axis_index("z"), lax.axis_index("core")]).astype(jnp.int32)
    piece = lax.axis_index("grp").astype(jnp.int32).reshape(1)
    slots = (place, src_block[0], dest_owner[:, 0], target, counts)
    half = ROWS // 2
    lower = panels[:, :, :half]
    upper = lax.optimization_barrier(panels)[:, :, half:]
    low_next, low_prev = over_y(lower, -1), over_y(lower, 1)
    up_next, up_prev = over_y(upper, -1), over_y(upper, 1)
    low_far = over_y(low_next, -1)
    up_far = over_y(up_prev, 1)
    rights = [(), (low_next, low_prev), (up_next, up_prev), (low_far, up_far)]
    summed = []
    for right in rights:
        packed = products(*slots, panels, right)
        arrived = [packed[0]] + [over_x(packed[d], d) for d in range(1, NX)]
        keep, other = combine(arrived)
        swapped = over_z(other, 0, 1)
        even, up, down = split(keep, swapped)
        parts = (even, over_z(up, 1, 0), over_z(down, -1, 0))
        merged = merge(parts)
        summed.append([merged[0]] + [over_z(merged[h], 2 * h, 0) for h in range(1, HOPS)])
    sofar = finish(piece, parent, summed[:3])
    return finish_last(piece, sofar, summed[3])


def solution(mesh):
    split = Mesh(mesh.devices.reshape(NY, NX, NZ, NC), ("grp", "x", "z", "core"))
    col = ("x", "z", "core")
    placed = (
        P(col, None, "grp", None),
        P(col, "grp", None),
        P(col, None),
        P(col, None),
        P(col),
        P(col),
    )
    return jax.shard_map(
        per_device, mesh=split, in_specs=placed, out_specs=P(col, "grp", None), check_vma=False
    )
```

```python
import functools

import jax
import jax.numpy as jnp
from jax import lax
from jax.experimental import pallas as pl
from jax.experimental.pallas import tpu as pltpu
from jax.sharding import Mesh, PartitionSpec as P


NX, NZ, NC, NY = 4, 8, 2, 4
FRONTS, BLOCKS, ROWS, WIDTH = 4, 4, 128, 512
PAIRS, SLOTS, TARGETS = 10, 40, 4
COLS = 128
SPOTS = NX * NC * NZ
LABEL_ROWS = 16
PER_X = NC * NZ
SENT_ROWS = PER_X * ROWS + LABEL_ROWS
VMEM = 12 * 1024 * 1024
SUM_ROWS = TARGETS * ROWS
HOPS = NZ // 2


def products_kernel(place, src, owner, target, count, left, *rest, parts):
    rights, outs, (made, pair_at, label_at) = rest[:parts], rest[parts:parts + NX], rest[-3:]
    x, z, core = place[0], place[1], place[2]
    live = count[0]

    def clear(i, carry):
        pair_at[i] = SLOTS
        label_at[i] = -1
        return carry

    lax.fori_loop(0, SPOTS + 1, clear, 0)

    def put(s, carry):
        o = owner[s]
        dx = (o // (NZ * NC) - x + NX) % NX
        dz = ((o // NC) % NZ - z + NZ) % NZ
        dc = (o % NC - core + NC) % NC
        spot = jnp.where(s < live, (dx * NC + dc) * NZ + dz, SPOTS)
        pair_at[spot] = src[s]
        label_at[spot] = target[s]
        return carry

    lax.fori_loop(0, SLOTS, put, 0)

    def piece(f, b):
        if parts == 0:
            return left[f, b]
        return jnp.concatenate([r[f, b] for r in rights], axis=0)

    def front(f, carry):
        for b in range(0, BLOCKS, 2):
            mine = left[f, b:].reshape((BLOCKS - b) * ROWS, WIDTH)
            right = jnp.concatenate([piece(f, b), piece(f, b + 1)], axis=0)
            product = lax.dot_general(
                mine, right, (((1,), (1,)), ((), ())), preferred_element_type=jnp.float32
            ).astype(jnp.bfloat16)
            for c in (b, b + 1):
                for a in range(c, BLOCKS):
                    at = pl.multiple_of((f * PAIRS + a * (a + 1) // 2 + c) * ROWS, ROWS)
                    made[pl.ds(at, ROWS), :] = product[(a - b) * ROWS:(a - b + 1) * ROWS, (c - b) * COLS:(c - b + 1) * COLS]
        return carry

    lax.fori_loop(0, FRONTS, front, 0)
    made[SLOTS * ROWS:, :] = jnp.zeros((ROWS, COLS), jnp.bfloat16)
    row = lax.broadcasted_iota(jnp.int32, (LABEL_ROWS, COLS), 0)
    for dx, out in enumerate(outs):
        tile = jnp.full((LABEL_ROWS, COLS), -1, jnp.int32)
        for i in range(PER_X):
            tile = jnp.where(row == i, label_at[dx * PER_X + i], tile)
        out[PER_X * ROWS:, :] = tile.astype(jnp.float32).astype(jnp.bfloat16)

        def place_block(i, carry, dx=dx, out=out):
            at = pl.multiple_of(pair_at[dx * PER_X + i] * ROWS, ROWS)
            out[pl.ds(pl.multiple_of(i * ROWS, ROWS), ROWS), :] = made[pl.ds(at, ROWS), :]
            return carry

        lax.fori_loop(0, PER_X, place_block, 0)


def products(place, src, owner, target, count, left, rights):
    smem = pl.BlockSpec(memory_space=pltpu.SMEM)
    whole = pl.BlockSpec(memory_space=pltpu.VMEM)
    parts = len(rights)
    return pl.pallas_call(
        functools.partial(products_kernel, parts=parts),
        in_specs=[smem] * 5 + [whole] * (1 + parts),
        out_specs=[whole] * NX,
        out_shape=[jax.ShapeDtypeStruct((SENT_ROWS, COLS), jnp.bfloat16)] * NX,
        scratch_shapes=[
            pltpu.VMEM(((SLOTS + 1) * ROWS, COLS), jnp.bfloat16),
            pltpu.SMEM((SPOTS + 1,), jnp.int32),
            pltpu.SMEM((SPOTS + 1,), jnp.int32),
        ],
        compiler_params=pltpu.CompilerParams(vmem_limit_bytes=VMEM),
        cost_estimate=pl.CostEstimate(
            flops=2 * SLOTS * ROWS * COLS * WIDTH, bytes_accessed=6 * 1024 * 1024, transcendentals=0),
        name="products",
    )(place, src, owner, target, count, left, *rights)


def combine_kernel(*refs):
    arrived, outs = refs[:NX], refs[NX:]
    step = 32
    tags = [a[PER_X * ROWS:SENT_ROWS, :].astype(jnp.float32) for a in arrived]
    for i in range(PER_X):
        tag = [jnp.broadcast_to(t[i:i + 1, :], (step, COLS)) for t in tags]

        def rows_of(r, carry, i=i, tag=tag, out=outs[i // NZ], start=i % NZ * SUM_ROWS):
            base = pl.multiple_of(r * step, step)
            sums = [jnp.zeros((step, COLS), jnp.float32) for _ in range(TARGETS)]
            for g in range(NX):
                v = arrived[g][pl.ds(i * ROWS + base, step), :].astype(jnp.float32)
                for t in range(TARGETS):
                    sums[t] = sums[t] + jnp.where(tag[g] == float(t), v, 0.0)
            for t in range(TARGETS):
                out[pl.ds(start + t * ROWS + base, step), :] = sums[t].astype(out.dtype)
            return carry

        lax.fori_loop(0, ROWS // step, rows_of, 0)


def in_vmem(kernel, inputs, shapes):
    whole = pl.BlockSpec(memory_space=pltpu.VMEM)
    return pl.pallas_call(
        kernel,
        in_specs=[whole] * len(inputs),
        out_specs=[whole] * len(shapes),
        out_shape=[jax.ShapeDtypeStruct((rows, COLS), dtype) for rows, dtype in shapes],
        compiler_params=pltpu.CompilerParams(vmem_limit_bytes=VMEM),
        cost_estimate=pl.CostEstimate(
            flops=8 * SPOTS * ROWS * COLS, bytes_accessed=3 * 1024 * 1024, transcendentals=0),
    )(*inputs)


def combine(arrived):
    rows = NZ * SUM_ROWS
    return in_vmem(combine_kernel, arrived, [(rows, jnp.float32), (rows, jnp.bfloat16)])


def split_kernel(keep, swapped, even, up, down):
    step = 64
    half = SUM_ROWS // 2

    def add(out, at, start, count):
        def rows_of(r, carry):
            base = pl.multiple_of(r * step, step)
            total = keep[pl.ds(start + base, step), :] + swapped[pl.ds(start + base, step), :].astype(jnp.float32)
            out[pl.ds(at + base, step), :] = total.astype(out.dtype)
            return carry

        lax.fori_loop(0, count // step, rows_of, 0)

    for dz in range(NZ):
        if dz % 2 == 0:
            add(even, dz // 2 * SUM_ROWS, dz * SUM_ROWS, SUM_ROWS)
        else:
            add(up, dz // 2 * half, dz * SUM_ROWS, half)
            add(down, (dz + 1) // 2 % HOPS * half, dz * SUM_ROWS + half, half)


def split(keep, swapped):
    rows = HOPS * SUM_ROWS
    return in_vmem(
        split_kernel, (keep, swapped),
        [(rows, jnp.float32), (rows // 2, jnp.bfloat16), (rows // 2, jnp.bfloat16)])


def merge_kernel(even, up, down, *outs):
    step = 64
    half = SUM_ROWS // 2
    for h, out in enumerate(outs):
        for part, moved in enumerate((up, down)):

            def rows_of(r, carry, h=h, out=out, part=part, moved=moved):
                base = pl.multiple_of(r * step, step)
                total = even[pl.ds(h * SUM_ROWS + part * half + base, step), :] + moved[
                    pl.ds(h * half + base, step), :].astype(jnp.float32)
                out[pl.ds(part * half + base, step), :] = total.astype(out.dtype)
                return carry

            lax.fori_loop(0, half // step, rows_of, 0)


def merge(parts):
    return in_vmem(
        merge_kernel, parts,
        [(SUM_ROWS, jnp.float32)] + [(SUM_ROWS, jnp.bfloat16)] * (HOPS - 1))


def block_sum(parts):
    total = parts[0][...].astype(jnp.float32)
    for p in parts[1:]:
        total = total + p[...].astype(jnp.float32)
    return total


def finish_kernel(piece, parent, *refs, sizes):
    out = refs[-1]
    sums, at = [], 0
    for n in sizes:
        sums.append(block_sum(refs[at:at + n]))
        at += n
    own, low, high = sums
    me, half = piece[0], COLS // 2
    values = {
        0: own,
        1: jnp.concatenate([low[:, :half], high[:, :half]], axis=1),
        2: None,
        3: jnp.concatenate([low[:, half:], high[:, half:]], axis=1),
    }
    for d, value in values.items():
        cols = pl.ds(pl.multiple_of(((me + d) % NY) * COLS, COLS), COLS)
        out[0, :, cols] = parent[0, :, cols] if value is None else parent[0, :, cols] - value


def finish(piece, parent, chunks):
    wide = pl.BlockSpec((1, ROWS, NY * COLS), lambda t: (t, 0, 0))
    flat = [part for chunk in chunks for part in chunk]
    return pl.pallas_call(
        functools.partial(finish_kernel, sizes=tuple(len(chunk) for chunk in chunks)),
        grid=(TARGETS,),
        in_specs=[pl.BlockSpec(memory_space=pltpu.SMEM), wide]
        + [pl.BlockSpec((ROWS, COLS), lambda t: (t, 0))] * len(flat),
        out_specs=wide,
        out_shape=jax.ShapeDtypeStruct(parent.shape, parent.dtype),
        compiler_params=pltpu.CompilerParams(
            dimension_semantics=("arbitrary",), vmem_limit_bytes=VMEM),
        cost_estimate=pl.CostEstimate(
            flops=30 * TARGETS * ROWS * COLS, bytes_accessed=5 * 1024 * 1024, transcendentals=0),
        name="finish",
    )(piece, parent, *flat)


def finish_last_kernel(piece, sofar, *refs):
    parts, (out, held, sem) = refs[:HOPS], refs[HOPS:]
    cols = pl.ds(pl.multiple_of((piece[0] + 2) % NY * COLS, COLS), COLS)
    load = pltpu.make_async_copy(sofar.at[:, :, cols], held, sem.at[0])
    load.start()
    load.wait()
    stores = []
    for t in range(TARGETS):
        held[t] = held[t] - block_sum([p.at[pl.ds(t * ROWS, ROWS)] for p in parts])
        stores.append(pltpu.make_async_copy(held.at[t], out.at[t, :, cols], sem.at[1 + t]))
        stores[-1].start()
    for c in stores:
        c.wait()


def finish_last(piece, sofar, chunk):
    hbm = pl.BlockSpec(memory_space=pl.ANY)
    return pl.pallas_call(
        finish_last_kernel,
        in_specs=[pl.BlockSpec(memory_space=pltpu.SMEM), hbm] + [pl.BlockSpec(memory_space=pltpu.VMEM)] * HOPS,
        out_specs=hbm,
        out_shape=jax.ShapeDtypeStruct(sofar.shape, sofar.dtype),
        scratch_shapes=[
            pltpu.VMEM((TARGETS, ROWS, COLS), jnp.float32),
            pltpu.SemaphoreType.DMA((1 + TARGETS,)),
        ],
        input_output_aliases={1: 0},
        compiler_params=pltpu.CompilerParams(vmem_limit_bytes=VMEM),
        cost_estimate=pl.CostEstimate(
            flops=10 * TARGETS * ROWS * COLS, bytes_accessed=2 * 1024 * 1024, transcendentals=0),
        name="finish_last",
    )(piece, sofar, *chunk)


def over_y(v, d):
    return lax.ppermute(v, "grp", [(i, (i + d) % NY) for i in range(NY)])


def over_x(v, dx):
    return lax.ppermute(v, "x", [(i, (i + dx) % NX) for i in range(NX)])


def over_z(v, dz, dc):
    pairs = [(z * NC + c, (z + dz) % NZ * NC + (c + dc) % NC) for z in range(NZ) for c in range(NC)]
    return lax.ppermute(v, ("z", "core"), pairs)


def per_device(panels, parent, src_block, dest_owner, target, counts):
    place = jnp.stack([lax.axis_index("x"), lax.axis_index("z"), lax.axis_index("core")]).astype(jnp.int32)
    piece = lax.axis_index("grp").astype(jnp.int32).reshape(1)
    slots = (place, src_block[0], dest_owner[:, 0], target, counts)
    half = ROWS // 2
    lower = panels[:, :, :half]
    upper = lax.optimization_barrier(panels)[:, :, half:]
    low_prev = over_y(lower, 1)
    low_next = over_y(lower, -1)
    up_prev = over_y(upper, 1)
    up_next = over_y(upper, -1)
    low_far = over_y(low_next, -1)
    up_far = over_y(up_prev, 1)
    rights = [(), (low_next, low_prev), (up_next, up_prev), (low_far, up_far)]
    summed = []
    for right in rights:
        packed = products(*slots, panels, right)
        arrived = [packed[0]] + [over_x(packed[d], d) for d in range(1, NX)]
        keep, other = combine(arrived)
        swapped = over_z(other, 0, 1)
        even, up, down = split(keep, swapped)
        parts = (even, over_z(up, 1, 0), over_z(down, -1, 0))
        merged = merge(parts)
        far = over_z(merged[2], 4, 0)
        summed.append([merged[0], over_z(merged[1], 2, 0), far, over_z(merged[3], -2, 0)])
    sofar = finish(piece, parent, summed[:3])
    return finish_last(piece, sofar, summed[3])


def solution(mesh):
    split = Mesh(mesh.devices.reshape(NY, NX, NZ, NC), ("grp", "x", "z", "core"))
    col = ("x", "z", "core")
    placed = (
        P(col, None, "grp", None),
        P(col, "grp", None),
        P(col, None),
        P(col, None),
        P(col),
        P(col),
    )
    return jax.shard_map(
        per_device, mesh=split, in_specs=placed, out_specs=P(col, "grp", None), check_vma=False
    )
```
